256 devices in a mesh: rep: 4 (over y, x), ep: 32 (over z), tp: 2 (over core).
Axes of the slice: x: 2, y: 2, z: 32, core: 2. Of those that a mesh axis runs over, the one named last changes fastest.
The devices are a block of a 4x8x32 slice.
Arguments:
- tokens: bfloat16 [8192, 3072], P(('rep', 'ep')), parts along dimension 0, may hold values from -6 to 6
- routes: int32 [8192, 2], P(('rep', 'ep')), parts along dimension 0, may hold values from 0 to 3, all different within a row; in each aligned block of 64 rows (0 to 63, 64 to 127, ...) at most 40 rows name the same one
- route_weight: float32 [8192, 2], P(('rep', 'ep')), parts along dimension 0, may hold values from 0.2 to 1
- gate_code: bfloat16 [3072, 32768], P(None, ('ep', 'tp')), may hold values from -0.109375 to 0.109375
- gate_scale: float32 [3072, 256], P(None, ('ep', 'tp')), may hold values from 0.5 to 2
- up_code: bfloat16 [3072, 32768], P(None, ('ep', 'tp')), may hold values from -0.109375 to 0.109375
- up_scale: float32 [3072, 256], P(None, ('ep', 'tp')), may hold values from 0.5 to 2
- down_code: bfloat16 [32768, 3072], P(('ep', 'tp')), may hold values from -0.0625 to 0.0625
- down_scale: float32 [32768, 24], P(('ep', 'tp')), may hold values from 0.5 to 2
Outputs:
- mixed: bfloat16 [8192, 3072], P(('rep', 'ep'), 'tp'), parts along dimension 0
The draws below stay inside these ranges and needn't reach their ends.
There are 4 independent parts, one for each index of `rep`. The reference program is written for one: setup_inputs(seed, part) draws one part's arguments, and reference() takes and returns one part's arrays. A program takes and returns all parts, laid end to end along the dimension named above; an argument that names none is the same for every part. Nothing has to cross between parts.
Inputs may be any that keep to these rules, and one draw needn't show every extreme that they name: `routes`: among the 64 rows of one index of ep, no expert is named by more than 40 rows, a bound that some block reaches; a row names 2 different experts.
All inputs are finite; a program needn't handle non-finite values.
Results may differ from the reference program's by a relative error of at most 0.02.
Values may be sent and summed in bfloat16 or wider, within the bound.
A program may use at most 128 MiB of HBM per device.

```python
import math
import jax
import jax.numpy as jnp
import numpy as np
from jax import lax

D = 3072
FF = 8192
EXPERTS = 4
TOP = 2
QB = 128
TOK_DEV = 64
CAP = 40
TOKENS = 2048
N_EP = 32


def levels(rng, shape, pieces, least, top_value):
    loudness = 1.0
    for axis_at, blocks in pieces:
        heights = jax.random.uniform(jax.random.fold_in(jax.random.fold_in(rng, 6), axis_at), (blocks,), jnp.float32, least / len(pieces), top_value / len(pieces))
        loudness = loudness * jnp.repeat(jnp.exp(heights), shape[axis_at] // blocks).reshape((-1,) + (1,) * (len(shape) - 1 - axis_at))
    return loudness


def deal_out(own_key, own, number, rows, count, top, bound, skew):
    order = jax.random.permutation(own_key, count)
    crowded, usual = load_shares(count, rows * top, bound, skew, True), load_shares(count, rows * top, bound, skew, False)
    places = jnp.arange(count)

    def named(sizes, turn):
        used = int((sizes > 0).sum())
        fixed = max(1, used // 4)
        moved = fixed + (places - fixed + turn * (used - fixed)) % max(1, count - fixed)
        return jnp.zeros((count,), jnp.int32).at[order[jnp.where(places < fixed, places, moved)]].set(jnp.asarray(sizes, jnp.int32))

    sizes = jnp.where(number % 4 == 0, named(crowded, number // 4), named(usual, number - number // 4 - 1))
    mixed = jax.random.permutation(jax.random.fold_in(own, 3), count)
    giver, receiver = mixed[0:count // 2 * 2:2], mixed[1:count // 2 * 2:2]
    slack = jnp.minimum(sizes[giver] - 1, bound - sizes[receiver]) // 2
    slack = jnp.where((giver == order[0]) | (receiver == order[0]) | (sizes[receiver] == 0), 0, jnp.maximum(slack, 0))
    moved = jax.random.randint(jax.random.fold_in(own, 4), (count // 2,), 0, 1 << 20) % (slack + 1)
    sizes = sizes.at[giver].add(-moved).at[receiver].add(moved)
    labels = jnp.searchsorted(jnp.cumsum(sizes), jnp.arange(rows * top), side="right").astype(jnp.int32)
    listing = labels.reshape(top, rows).T
    listing = listing[jax.random.permutation(jax.random.fold_in(own, 1), rows)]
    turn = jax.random.randint(jax.random.fold_in(own, 2), (rows, 1), 0, top)
    return jnp.take_along_axis(listing, (jnp.arange(top)[None, :] + turn) % top, axis=1)


def load_shares(count, total, limit, lean, full):
    loads = [(1 << 20) // math.isqrt(standing ** lean) + 1 for standing in range(1, count + 1)]
    largest = limit if full else min(limit, max(-(-total // count), total * loads[0] // sum(loads)))
    least = 1 if total - largest >= count - 1 else 0
    given, surplus = [largest] + [least] * (count - 1), total - largest - least * (count - 1)
    while surplus > 0:
        movable = [i for i in range(1, count) if given[i] < largest] or [i for i in range(1, count) if given[i] < limit]
        pool, left = sum([loads[i] for i in movable]), surplus
        for i in movable:
            extra = min(limit - given[i], max(1, left * loads[i] // pool), surplus)
            given[i] = given[i] + extra
            surplus = surplus - extra
    return np.array(given)


def scatter_about(key, shape, width, limit, shards=(), held_as=jnp.bfloat16):
    level = levels(key, shape, shards, -0.22, 0.18) if shards else 1.0
    values = jax.random.normal(key, shape, jnp.float32) * width * level
    return jnp.minimum(jnp.maximum(values, -limit), limit).astype(held_as)


def setup_inputs(seed: int = 0, part: int = 0) -> dict:
    key_of = jax.random.split(jax.random.key(seed), 10)
    part_keys = jax.random.split(jax.random.fold_in(key_of[9], part), 10)
    tokens = scatter_about(part_keys[0], (TOKENS, D), 1.0, 6.0, ((0, 32),))
    routes_keys = jax.random.split(jax.random.fold_in(part_keys[1], 1), TOKENS // TOK_DEV)
    routes_turns = jax.random.permutation(jax.random.fold_in(part_keys[1], 3), TOKENS // TOK_DEV)
    routes = jax.vmap(lambda own, number: deal_out(jax.random.fold_in(part_keys[1], 2), own, number, TOK_DEV, EXPERTS, TOP, CAP, 2))(routes_keys, routes_turns).reshape((TOKENS, TOP))
    route_weight = jnp.clip(0.2 + 0.8 * jax.random.uniform(part_keys[2], (TOKENS, TOP), jnp.float32) ** levels(part_keys[2], (TOKENS, TOP), ((0, 32),), -0.2, 0.2), 0.2, 1.0)
    gate_code = scatter_about(key_of[3], (D, EXPERTS * FF), D ** -0.5, 0.109375, ((1, 64),))
    gate_scale = jnp.clip(jnp.exp(math.log(2.0) - 1.3862944 * jax.random.uniform(key_of[4], (D, EXPERTS * FF // QB), jnp.float32) ** levels(key_of[4], (D, EXPERTS * FF // QB), ((1, 64),), -0.2, 0.2)), 0.5, 2.0)
    up_code = scatter_about(key_of[5], (D, EXPERTS * FF), D ** -0.5, 0.109375, ((1, 64),))
    up_scale = jnp.clip(jnp.exp(math.log(2.0) - 1.3862944 * jax.random.uniform(key_of[6], (D, EXPERTS * FF // QB), jnp.float32) ** levels(key_of[6], (D, EXPERTS * FF // QB), ((1, 64),), -0.2, 0.2)), 0.5, 2.0)
    down_code = scatter_about(key_of[7], (EXPERTS * FF, D), FF ** -0.5, 0.0625, ((0, 64),))
    down_scale = jnp.clip(jnp.exp(math.log(2.0) - 1.3862944 * jax.random.uniform(key_of[8], (EXPERTS * FF, D // QB), jnp.float32) ** levels(key_of[8], (EXPERTS * FF, D // QB), ((0, 64),), -0.2, 0.2)), 0.5, 2.0)
    return dict(tokens=tokens, routes=routes, route_weight=route_weight, gate_code=gate_code, gate_scale=gate_scale, up_code=up_code, up_scale=up_scale, down_code=down_code, down_scale=down_scale)


def dequant(code, scale):
    return (code.astype(jnp.float32) * jnp.repeat(scale, QB, axis=1)).astype(jnp.bfloat16)


def slot_table(expert_ids):
    onehot = (expert_ids[:, None] == jnp.arange(EXPERTS, dtype=jnp.int32)[None, :]).astype(jnp.int32)
    before = jnp.cumsum(onehot, axis=0) - onehot
    return jnp.sum(before * onehot, axis=1).astype(jnp.int32)


def reference(tokens, routes, route_weight, gate_code, gate_scale, up_code, up_scale, down_code, down_scale):
    token_blocks = tokens.reshape(N_EP, TOK_DEV, D)
    expert_ids = routes.reshape(N_EP, TOK_DEV * TOP)
    pair_weight = route_weight.reshape(N_EP, TOK_DEV * TOP)
    slot_rank = jax.vmap(slot_table)(expert_ids)
    target = expert_ids * CAP + slot_rank
    columns = jnp.arange(EXPERTS * CAP, dtype=jnp.int32)
    picked = (target[:, None, :] == columns[None, :, None]).astype(jnp.float32)
    repeated = jnp.repeat(token_blocks, TOP, axis=1).astype(jnp.float32)
    buffers = jnp.einsum("scp,spd->scd", picked, repeated).astype(jnp.bfloat16)
    buffers = buffers.reshape(N_EP, EXPERTS, CAP, D)
    outputs = []
    for expert in range(EXPERTS):
        low = expert * FF
        w_gate = dequant(gate_code[:, low:low + FF], gate_scale[:, low // QB:(low + FF) // QB])
        w_up = dequant(up_code[:, low:low + FF], up_scale[:, low // QB:(low + FF) // QB])
        w_down = dequant(down_code[low:low + FF, :], down_scale[low:low + FF, :])
        expert_rows = buffers[:, expert].reshape(N_EP * CAP, D)
        gate_act = jnp.dot(expert_rows, w_gate, preferred_element_type=jnp.float32)
        up_act = jnp.dot(expert_rows, w_up, preferred_element_type=jnp.float32)
        hidden = (jax.nn.silu(gate_act) * up_act).astype(jnp.bfloat16)
        result = jnp.dot(hidden, w_down, preferred_element_type=jnp.float32)
        outputs.append(result.reshape(N_EP, CAP, D))
    stacked = jnp.stack(outputs, axis=1).reshape(N_EP, EXPERTS * CAP, D)
    mixing = jnp.where(target[:, :, None] == columns[None, None, :], pair_weight[:, :, None], 0.0)
    mixing = mixing.astype(jnp.float32).reshape(N_EP, TOK_DEV, TOP, EXPERTS * CAP).sum(axis=2)
    mixed = jnp.einsum("spc,scd->spd", mixing, stacked, precision=lax.Precision.HIGHEST)
    return mixed.reshape(TOKENS, D).astype(jnp.bfloat16)
```

```python
import functools

import jax
import jax.numpy as jnp
from jax import lax
from jax.experimental import pallas as pl
from jax.experimental.pallas import tpu as pltpu
from jax.sharding import PartitionSpec as P

EXPERTS = 4
QB = 128
CHUNKS = 4
MESH = pl.DeviceIdType.MESH


def kernel(
    n,
    tokens, routes, weights, gate_code, gate_scale, up_code, up_scale, down_code, down_scale,
    out,
    rows, part, theirs, sums, w_gate, w_up, w_down, s_gate, s_up, s_down,
    hidden, coef, swap_out, swap_in,
    load_sem, ag_send, ag_recv, cf_send, cf_recv, sw_send, sw_recv, sc_send, sc_recv,
    po_send, po_recv, rs_send, rs_recv, fx_send, fx_recv,
):
    steps = n // 2
    count = rows.shape[1] // 2
    half = count // 2
    width = rows.shape[2]
    span = width // CHUNKS
    units = w_gate.shape[1]
    last = steps - 1

    ep = lax.axis_index("ep")
    tp = lax.axis_index("tp")
    toward = 1 - 2 * tp
    ahead = {"ep": lax.rem(ep + toward + n, n)}
    behind = {"ep": lax.rem(ep - toward + n, n)}
    partner = {"tp": 1 - tp}
    expert = ep // (n // EXPERTS)
    own_half = pl.multiple_of(half * tp, half)
    other_half = pl.multiple_of(half * (1 - tp), half)

    def send(src, dst, send_sem, recv_sem, where):
        return pltpu.make_async_remote_copy(
            src_ref=src, dst_ref=dst, send_sem=send_sem, recv_sem=recv_sem,
            device_id=where, device_id_type=MESH,
        )

    own = rows.at[last, pl.ds(count, count)]

    def gather(k, f):
        cols = pl.ds(f * span, span)
        if isinstance(k, int) and k == 1:
            src = own.at[:, cols]
        else:
            src = rows.at[k - 2, pl.ds(0, count), cols]
        return send(
            src, rows.at[k - 1, pl.ds(0, count), cols],
            ag_send.at[lax.rem(k, 2), f], ag_recv.at[k - 1, f], ahead,
        )

    def gather_half(f):
        cols = pl.ds(f * span, span)
        return send(
            rows.at[last - 1, pl.ds(own_half, half), cols], rows.at[last, pl.ds(0, half), cols],
            ag_send.at[steps % 2, f], ag_recv.at[last, f], ahead,
        )

    def gather_coef(k):
        src = coef.at[last, 1] if isinstance(k, int) and k == 1 else coef.at[k - 2, 0]
        return send(
            src, coef.at[k - 1, 0], cf_send.at[lax.rem(k, 2)], cf_recv.at[k - 1], ahead
        )

    def swap(k):
        return send(
            rows.at[k - 1, pl.ds(0, count)], rows.at[k - 1, pl.ds(count, count)],
            sw_send.at[lax.rem(k, 2)], sw_recv.at[k - 1], partner,
        )

    def swap_half():
        return send(
            rows.at[last, pl.ds(0, half)], rows.at[last, pl.ds(half, half)],
            sw_send.at[steps % 2], sw_recv.at[last], partner,
        )

    def swap_coef(k):
        return send(
            coef.at[k - 1, 0], coef.at[k - 1, 1],
            sc_send.at[lax.rem(k, 2)], sc_recv.at[k - 1], partner,
        )

    def hand(k):
        return send(
            part.at[k - 1, pl.ds(count, count)], theirs.at[k - 1],
            po_send.at[lax.rem(k, 2)], po_recv.at[k - 1], partner,
        )

    def hand_half(q):
        cols = pl.ds(q * (width // 2), width // 2)
        return send(
            part.at[last, pl.ds(half, half), cols], theirs.at[last, pl.ds(0, half), cols],
            po_send.at[2 + q], po_recv.at[last + q], partner,
        )

    def column(f):
        chunk = lax.rem(2 * (1 - tp) + f, CHUNKS)
        return pl.ds(pl.multiple_of(chunk * span, span), span)

    def reduce(j, f):
        return send(
            part.at[last - j, pl.ds(0, count), column(f)], sums.at[j, :, column(f)],
            rs_send.at[lax.rem(j, 2), f], rs_recv.at[j, f], behind,
        )

    def reduce_first(f):
        return send(
            part.at[last, pl.ds(0, half), column(f)],
            sums.at[0, pl.ds(own_half, half), column(f)],
            rs_send.at[0, f], rs_recv.at[0, f], behind,
        )

    def finish(i):
        cols = pl.ds(i * span, span)
        return send(
            swap_out.at[:, cols], swap_in.at[:, cols], fx_send.at[i], fx_recv.at[i], partner
        )

    def when(test, do):
        if isinstance(test, bool):
            if test:
                do()
        else:
            pl.when(test)(do)

    loads = [
        pltpu.make_async_copy(src, dst, load_sem.at[i])
        for i, (src, dst) in enumerate((
            (tokens, own), (gate_scale, s_gate), (gate_code, w_gate), (up_scale, s_up),
            (up_code, w_up), (down_scale, s_down), (down_code, w_down),
        ))
    ]
    for load in loads:
        load.start()

    barrier = pltpu.get_barrier_semaphore()
    for device in (ahead, behind, partner):
        pl.semaphore_signal(barrier, inc=1, device_id=device, device_id_type=MESH)

    names = lax.broadcasted_iota(jnp.int32, (8, count), 0)
    mine = jnp.where(names == routes[0:1, :], weights[0:1, :], 0.0)
    mine += jnp.where(names == routes[1:2, :], weights[1:2, :], 0.0)
    coef[last, 1] = jnp.concatenate((mine, jnp.zeros((8, 128 - count), jnp.float32)), axis=1)
    loads[0].wait()
    pl.semaphore_wait(barrier, 3)

    for f in range(CHUNKS):
        gather(1, f).start()
    gather_coef(1).start()

    def poll(k, f):
        def full():
            gather(k, f).wait_recv()
            if isinstance(k, int):
                if k >= 2:
                    gather(k - 1, f).wait_send()
                gather(k + 1, f).start()
                return

            @pl.when(k < last)
            def _():
                gather(k - 1, f).wait_send()
                gather(k + 1, f).start()

            @pl.when(k == last)
            def _():
                gather(k - 1, f).wait_send()
                gather_half(f).start()

        def weights_too():
            gather_coef(k).wait_recv()

            def onward():
                if not isinstance(k, int) or k >= 2:
                    gather_coef(k - 1).wait_send()
                gather_coef(k + 1).start()

            when(k < steps, onward)

        def across():
            if not isinstance(k, int) or k >= 3:
                swap(k - 2).wait_send()
                swap_coef(k - 2).wait_send()
            swap(k).start()
            swap_coef(k).start()

        def across_half():
            swap(steps - 2).wait_send()
            swap_half().start()

        when(k < steps, full)
        when(k == steps, lambda: gather_half(f).wait_recv())
        if f == 0:
            when(k <= steps, weights_too)
        if f == CHUNKS - 1:
            when(k < steps, across)
            when(k == steps, across_half)

    def dequant(code, scale, base):
        blocks = code.shape[1] // QB
        grid = scale[:, pl.ds(base, QB)]
        if blocks % 8:
            pad = jnp.zeros((8 - blocks % 8, QB), jnp.float32)
            grid = jnp.concatenate((grid, pad), axis=0)
        grid = grid.T
        for b in range(blocks):
            at = (pl.ds(base, QB), pl.ds(b * QB, QB))
            code[at] = (code[at].astype(jnp.float32) * grid[:, b : b + 1]).astype(code.dtype)

    def dequant_piece(m, f):
        code, scale = ((w_gate, s_gate), (w_up, s_up), (w_down, s_down))[m]
        size = code.shape[0] // CHUNKS

        @pl.loop(0, size // QB)
        def _(r):
            dequant(code, scale, pl.multiple_of(f * size + r * QB, QB))

    def arrived(k):
        def full():
            swap(k).wait_recv()
            swap_coef(k).wait_recv()

        when(k < steps, full)
        when(k == steps, lambda: swap_half().wait_recv())

    def factors(k):
        shift = jnp.where(k == steps, half * tp, 0)
        token = lax.broadcasted_iota(jnp.int32, (count, 128), 0)
        lane = lax.broadcasted_iota(jnp.int32, (count, 128), 1)
        line = coef[k - 1, 0, pl.ds(expert, 1), :]
        first = jnp.sum(
            jnp.where(lane == ((token + shift) & (count - 1)), line, 0.0), axis=1, keepdims=True
        )
        line = coef[k - 1, 1, pl.ds(expert, 1), :]
        second = jnp.sum(jnp.where(lane == token, line, 0.0), axis=1, keepdims=True)
        return jnp.concatenate((first, second), axis=0)

    def widen(k, p):
        cols = pl.ds(p * (units // 2), units // 2)
        x = rows[k - 1]
        gate = jnp.dot(x, w_gate[:, cols], preferred_element_type=jnp.float32)
        up = jnp.dot(x, w_up[:, cols], preferred_element_type=jnp.float32)
        small = jnp.exp(-jnp.abs(gate))
        silu = gate * (jnp.where(gate >= 0, 1.0, small) / (1.0 + small))
        hidden[:, cols] = (silu * up * factors(k)).astype(hidden.dtype)

    def narrow(k, q):
        cols = pl.ds(q * (width // 2), width // 2)
        got = jnp.dot(hidden[...], w_down[:, cols], preferred_element_type=jnp.float32)
        part[k - 1, :, cols] = got.astype(part.dtype)
        when(k == steps, lambda: hand_half(q).start())
        if q == 1:

            def whole():
                def free():
                    hand(k - 2).wait_send()

                when(k >= 3, free)
                hand(k).start()

            when(k < steps, whole)

    def pieces(k):
        return [
            lambda: arrived(k),
            functools.partial(widen, k, 0),
            functools.partial(widen, k, 1),
            functools.partial(narrow, k, 0),
            functools.partial(narrow, k, 1),
        ]

    for k in range(1, 4):
        loads[2 * k - 1].wait()
        loads[2 * k].wait()
        for f in range(CHUNKS):
            poll(k, f)
            dequant_piece(k - 1, f)

    @pl.loop(4, 6)
    def _(k):
        todo = pieces(2 * k - 7) + pieces(2 * k - 6)
        poll(k, 0)
        for do in todo[0:3]:
            do()
        poll(k, 1)
        for do in todo[3:5]:
            do()
        poll(k, 2)
        for do in todo[5:8]:
            do()
        poll(k, 3)
        for do in todo[8:10]:
            do()

    @pl.loop(6, steps + 2)
    def _(k):
        ready, *todo = pieces(k - 1)
        for f in range(CHUNKS):
            poll(k, f)
            if f == 0:
                ready()
            todo[f]()

    def wide(ref):
        return ref.astype(jnp.float32)

    for f in range(CHUNKS):
        if f == 0:
            hand_half(0).wait_recv()
            hand_half(1).wait_recv()
        cols = column(f)
        part[last, pl.ds(0, half), cols] = (
            wide(part[last, pl.ds(0, half), cols]) + wide(theirs[last, pl.ds(0, half), cols])
        ).astype(part.dtype)
        reduce_first(f).start()

    hand(last).wait_recv()
    for f in range(CHUNKS):
        cols = column(f)
        at, rest = pl.ds(own_half, half), pl.ds(other_half, half)
        part[last - 1, rest, cols] = (
            wide(part[last - 1, rest, cols]) + wide(theirs[last - 1, rest, cols])
        ).astype(part.dtype)
        reduce_first(f).wait_recv()
        part[last - 1, at, cols] = (
            wide(part[last - 1, at, cols])
            + wide(theirs[last - 1, at, cols])
            + wide(sums[0, at, cols])
        ).astype(part.dtype)
        reduce(1, f).start()

    @pl.loop(2, steps)
    def _(j):
        k = last - j
        hand(k + 1).wait_recv()
        for f in range(CHUNKS):
            cols = column(f)
            base = wide(part[k, pl.ds(0, count), cols]) + wide(theirs[k, :, cols])
            reduce(j - 1, f).wait_recv()
            part[k, pl.ds(0, count), cols] = (base + wide(sums[j - 1, :, cols])).astype(part.dtype)

            @pl.when(j == 2)
            def _():
                reduce_first(f).wait_send()

            @pl.when(j > 2)
            def _():
                reduce(j - 2, f).wait_send()

            reduce(j, f).start()

    for f in range(CHUNKS):
        cols = column(f)
        base = wide(part[last, pl.ds(count, count), cols])
        reduce(last, f).wait_recv()
        total = base + wide(sums[last, :, cols])
        if f < CHUNKS // 2:
            swap_out[:, f * span : (f + 1) * span] = total.astype(swap_out.dtype)
            finish(f).start()
        else:
            i = f - CHUNKS // 2
            at = slice(i * span, (i + 1) * span)
            finish(i).wait_recv()
            out[:, at] = (total + wide(swap_in[:, at])).astype(out.dtype)

    for f in range(CHUNKS):
        gather(last, f).wait_send()
        gather_half(f).wait_send()
        reduce(last - 1, f).wait_send()
        reduce(last, f).wait_send()
    gather_coef(last).wait_send()
    gather_coef(steps).wait_send()
    swap(last).wait_send()
    swap_half().wait_send()
    swap_coef(last - 1).wait_send()
    swap_coef(last).wait_send()
    hand(last - 1).wait_send()
    hand(last).wait_send()
    for q in range(2):
        hand_half(q).wait_send()
        finish(q).wait_send()


def local(
    n, tokens, routes, route_weight, gate_code, gate_scale, up_code, up_scale, down_code, down_scale
):
    steps = n // 2
    count, width = tokens.shape
    units = gate_code.shape[1]
    vmem = pl.BlockSpec(memory_space=pltpu.VMEM)
    far = pl.BlockSpec(memory_space=pl.ANY)
    bf16, f32 = jnp.bfloat16, jnp.float32
    dma = pltpu.SemaphoreType.DMA
    return pl.pallas_call(
        functools.partial(kernel, n),
        out_shape=jax.ShapeDtypeStruct((count, width // 2), bf16),
        in_specs=[far, vmem, vmem, far, far, far, far, far, far],
        out_specs=vmem,
        scratch_shapes=[
            pltpu.VMEM((steps, 2 * count, width), bf16),
            pltpu.VMEM((steps, 2 * count, width), bf16),
            pltpu.VMEM((steps, count, width), bf16),
            pltpu.VMEM((steps, count, width), bf16),
            pltpu.VMEM(gate_code.shape, bf16),
            pltpu.VMEM(up_code.shape, bf16),
            pltpu.VMEM(down_code.shape, bf16),
            pltpu.VMEM(gate_scale.shape[::-1], f32),
            pltpu.VMEM(up_scale.shape[::-1], f32),
            pltpu.VMEM(down_scale.shape[::-1], f32),
            pltpu.VMEM((2 * count, units), bf16),
            pltpu.VMEM((steps, 2, 8, 128), f32),
            pltpu.VMEM((count, width // 2), bf16),
            pltpu.VMEM((count, width // 2), bf16),
            dma((7,)),
            dma((2, CHUNKS)),
            dma((steps, CHUNKS)),
            dma((2,)),
            dma((steps,)),
            dma((2,)),
            dma((steps,)),
            dma((2,)),
            dma((steps,)),
            dma((4,)),
            dma((steps + 1,)),
            dma((2, CHUNKS)),
            dma((steps, CHUNKS)),
            dma((2,)),
            dma((2,)),
        ],
        compiler_params=pltpu.CompilerParams(
            collective_id=0, has_side_effects=True, vmem_limit_bytes=62 << 20
        ),
    )(
        tokens, routes.T, route_weight.T, gate_code, gate_scale.T, up_code, up_scale.T,
        down_code, down_scale.T,
    )


def solution(mesh):
    placed = (
        P(("rep", "ep"), None),
        P(("rep", "ep"), None),
        P(("rep", "ep"), None),
        P(None, ("ep", "tp")),
        P(None, ("ep", "tp")),
        P(None, ("ep", "tp")),
        P(None, ("ep", "tp")),
        P(("ep", "tp"), None),
        P(("ep", "tp"), None),
    )
    return jax.shard_map(
        functools.partial(local, mesh.shape["ep"]),
        mesh=mesh,
        in_specs=placed,
        out_specs=P(("rep", "ep"), "tp"),
        check_vma=False,
    )
```

```python
import functools

import jax
import jax.numpy as jnp
from jax import lax
from jax.experimental import pallas as pl
from jax.experimental.pallas import tpu as pltpu
from jax.sharding import PartitionSpec as P

EXPERTS = 4
QB = 128
CHUNKS = 8
PIECES = 4
MESH = pl.DeviceIdType.MESH


def kernel(
    n,
    tokens, routes, weights, gate_code, gate_scale, up_code, up_scale, down_code, down_scale,
    out,
    rows, part, theirs, sums, w_gate, w_up, w_down, s_gate, s_up, s_down,
    hidden, coef, swap_out, swap_in,
    load_sem, ag_send, ag_recv, cf_send, cf_recv, sw_send, sw_recv, sc_send, sc_recv,
    po_send, po_recv, rs_send, rs_recv, fx_send, fx_recv,
):
    steps = n // 2
    count = rows.shape[1] // 2
    half = count // 2
    width = rows.shape[2]
    span = width // CHUNKS
    units = w_gate.shape[1]
    last = steps - 1

    ep = lax.axis_index("ep")
    tp = lax.axis_index("tp")
    toward = 1 - 2 * tp
    ahead = {"ep": lax.rem(ep + toward + n, n)}
    behind = {"ep": lax.rem(ep - toward + n, n)}
    partner = {"tp": 1 - tp}
    expert = ep // (n // EXPERTS)
    own_half = pl.multiple_of(half * tp, half)
    other_half = pl.multiple_of(half * (1 - tp), half)

    def send(src, dst, send_sem, recv_sem, where):
        return pltpu.make_async_remote_copy(
            src_ref=src, dst_ref=dst, send_sem=send_sem, recv_sem=recv_sem,
            device_id=where, device_id_type=MESH,
        )

    own = rows.at[last, pl.ds(count, count)]

    def gather(k, f):
        cols = pl.ds(f * span, span)
        if isinstance(k, int) and k == 1:
            src = own.at[:, cols]
        else:
            src = rows.at[k - 2, pl.ds(0, count), cols]
        return send(
            src, rows.at[k - 1, pl.ds(0, count), cols],
            ag_send.at[lax.rem(k, 2), f], ag_recv.at[k - 1, f], ahead,
        )

    def gather_half(f):
        cols = pl.ds(f * span, span)
        return send(
            rows.at[last - 1, pl.ds(own_half, half), cols], rows.at[last, pl.ds(0, half), cols],
            ag_send.at[steps % 2, f], ag_recv.at[last, f], ahead,
        )

    def gather_coef(k):
        src = coef.at[last, 1] if isinstance(k, int) and k == 1 else coef.at[k - 2, 0]
        return send(
            src, coef.at[k - 1, 0], cf_send.at[lax.rem(k, 2)], cf_recv.at[k - 1], ahead
        )

    def swap(k):
        return send(
            rows.at[k - 1, pl.ds(0, count)], rows.at[k - 1, pl.ds(count, count)],
            sw_send.at[lax.rem(k, 2)], sw_recv.at[k - 1], partner,
        )

    def swap_half():
        return send(
            rows.at[last, pl.ds(0, half)], rows.at[last, pl.ds(half, half)],
            sw_send.at[steps % 2], sw_recv.at[last], partner,
        )

    def swap_coef(k):
        return send(
            coef.at[k - 1, 0], coef.at[k - 1, 1],
            sc_send.at[lax.rem(k, 2)], sc_recv.at[k - 1], partner,
        )

    def hand(k):
        return send(
            part.at[k - 1, pl.ds(count, count)], theirs.at[k - 1],
            po_send.at[lax.rem(k, 2)], po_recv.at[k - 1], partner,
        )

    def hand_half(q):
        cols = pl.ds(q * (width // 2), width // 2)
        return send(
            part.at[last, pl.ds(half, half), cols], theirs.at[last, pl.ds(0, half), cols],
            po_send.at[2 + q], po_recv.at[last + q], partner,
        )

    def column(f):
        chunk = lax.rem(CHUNKS // 2 * (1 - tp) + f, CHUNKS)
        return pl.ds(pl.multiple_of(chunk * span, span), span)

    def reduce(j, f):
        return send(
            part.at[last - j, pl.ds(0, count), column(f)], sums.at[j, :, column(f)],
            rs_send.at[lax.rem(j, 2), f], rs_recv.at[j, f], behind,
        )

    def reduce_first(f):
        return send(
            part.at[last, pl.ds(0, half), column(f)],
            sums.at[0, pl.ds(own_half, half), column(f)],
            rs_send.at[0, f], rs_recv.at[0, f], behind,
        )

    def finish(i):
        cols = pl.ds(i * span, span)
        return send(
            swap_out.at[:, cols], swap_in.at[:, cols], fx_send.at[i], fx_recv.at[i], partner
        )

    def when(test, do):
        if isinstance(test, bool):
            if test:
                do()
        else:
            pl.when(test)(do)

    loads = [
        pltpu.make_async_copy(src, dst, load_sem.at[i])
        for i, (src, dst) in enumerate((
            (tokens, own), (gate_scale, s_gate), (gate_code, w_gate), (up_scale, s_up),
            (up_code, w_up), (down_scale, s_down), (down_code, w_down),
        ))
    ]
    for load in loads:
        load.start()

    barrier = pltpu.get_barrier_semaphore()
    for device in (ahead, behind, partner):
        pl.semaphore_signal(barrier, inc=1, device_id=device, device_id_type=MESH)

    names = lax.broadcasted_iota(jnp.int32, (8, count), 0)
    mine = jnp.where(names == routes[0:1, :], weights[0:1, :], 0.0)
    mine += jnp.where(names == routes[1:2, :], weights[1:2, :], 0.0)
    coef[last, 1] = jnp.concatenate((mine, jnp.zeros((8, 128 - count), jnp.float32)), axis=1)
    loads[0].wait()
    pl.semaphore_wait(barrier, 3)

    for f in range(CHUNKS):
        gather(1, f).start()
    gather_coef(1).start()

    def poll(k, f):
        def full():
            gather(k, f).wait_recv()
            if isinstance(k, int):
                if k >= 2:
                    gather(k - 1, f).wait_send()
                gather(k + 1, f).start()
                return

            @pl.when(k < last)
            def _():
                gather(k - 1, f).wait_send()
                gather(k + 1, f).start()

            @pl.when(k == last)
            def _():
                gather(k - 1, f).wait_send()
                gather_half(f).start()

        def weights_too():
            gather_coef(k).wait_recv()

            def onward():
                if not isinstance(k, int) or k >= 2:
                    gather_coef(k - 1).wait_send()
                gather_coef(k + 1).start()

            when(k < steps, onward)

        def across():
            if not isinstance(k, int) or k >= 3:
                swap(k - 2).wait_send()
                swap_coef(k - 2).wait_send()
            swap(k).start()
            swap_coef(k).start()

        def across_half():
            swap(steps - 2).wait_send()
            swap_half().start()

        when(k < steps, full)
        when(k == steps, lambda: gather_half(f).wait_recv())
        if f == 0:
            when(k <= steps, weights_too)
        if f == CHUNKS - 1:
            when(k < steps, across)
            when(k == steps, across_half)

    def polls(k, p):
        for f in range(CHUNKS // PIECES):
            poll(k, p * (CHUNKS // PIECES) + f)

    def dequant(code, scale, base):
        blocks = code.shape[1] // QB
        grid = scale[:, pl.ds(base, QB)]
        if blocks % 8:
            pad = jnp.zeros((8 - blocks % 8, QB), jnp.float32)
            grid = jnp.concatenate((grid, pad), axis=0)
        grid = grid.T
        for b in range(blocks):
            at = (pl.ds(base, QB), pl.ds(b * QB, QB))
            code[at] = (code[at].astype(jnp.float32) * grid[:, b : b + 1]).astype(code.dtype)

    def dequant_piece(m, f):
        code, scale = ((w_gate, s_gate), (w_up, s_up), (w_down, s_down))[m]
        size = code.shape[0] // PIECES

        @pl.loop(0, size // QB)
        def _(r):
            dequant(code, scale, pl.multiple_of(f * size + r * QB, QB))

    def arrived(k):
        def full():
            swap(k).wait_recv()
            swap_coef(k).wait_recv()

        when(k < steps, full)
        when(k == steps, lambda: swap_half().wait_recv())

    def factors(k):
        shift = jnp.where(k == steps, half * tp, 0)
        token = lax.broadcasted_iota(jnp.int32, (count, 128), 0)
        lane = lax.broadcasted_iota(jnp.int32, (count, 128), 1)
        line = coef[k - 1, 0, pl.ds(expert, 1), :]
        first = jnp.sum(
            jnp.where(lane == ((token + shift) & (count - 1)), line, 0.0), axis=1, keepdims=True
        )
        line = coef[k - 1, 1, pl.ds(expert, 1), :]
        second = jnp.sum(jnp.where(lane == token, line, 0.0), axis=1, keepdims=True)
        return jnp.concatenate((first, second), axis=0)

    def widen(k, p):
        cols = pl.ds(p * (units // 2), units // 2)
        x = rows[k - 1]
        gate = jnp.dot(x, w_gate[:, cols], preferred_element_type=jnp.float32)
        up = jnp.dot(x, w_up[:, cols], preferred_element_type=jnp.float32)
        small = jnp.exp(-jnp.abs(gate))
        silu = gate * (jnp.where(gate >= 0, 1.0, small) / (1.0 + small))
        hidden[:, cols] = (silu * up * factors(k)).astype(hidden.dtype)

    def narrow(k, q):
        cols = pl.ds(q * (width // 2), width // 2)
        got = jnp.dot(hidden[...], w_down[:, cols], preferred_element_type=jnp.float32)
        part[k - 1, :, cols] = got.astype(part.dtype)
        when(k == steps, lambda: hand_half(q).start())
        if q == 1:

            def whole():
                def free():
                    hand(k - 2).wait_send()

                when(k >= 3, free)
                hand(k).start()

            when(k < steps, whole)

    def pieces(k):
        return [
            lambda: arrived(k),
            functools.partial(widen, k, 0),
            functools.partial(widen, k, 1),
            functools.partial(narrow, k, 0),
            functools.partial(narrow, k, 1),
        ]

    for k in range(1, 4):
        loads[2 * k - 1].wait()
        loads[2 * k].wait()
        for p in range(PIECES):
            polls(k, p)
            dequant_piece(k - 1, p)

    @pl.loop(4, 6)
    def _(k):
        todo = pieces(2 * k - 7) + pieces(2 * k - 6)
        polls(k, 0)
        for do in todo[0:3]:
            do()
        polls(k, 1)
        for do in todo[3:5]:
            do()
        polls(k, 2)
        for do in todo[5:8]:
            do()
        polls(k, 3)
        for do in todo[8:10]:
            do()

    @pl.loop(6, steps + 2)
    def _(k):
        ready, *todo = pieces(k - 1)
        for p in range(PIECES):
            polls(k, p)
            if p == 0:
                ready()
            todo[p]()

    def wide(ref):
        return ref.astype(jnp.float32)

    for f in range(CHUNKS):
        if f == 0:
            hand_half(0).wait_recv()
            hand_half(1).wait_recv()
        cols = column(f)
        part[last, pl.ds(0, half), cols] = (
            wide(part[last, pl.ds(0, half), cols]) + wide(theirs[last, pl.ds(0, half), cols])
        ).astype(part.dtype)
        reduce_first(f).start()

    hand(last).wait_recv()
    for f in range(CHUNKS):
        cols = column(f)
        at, rest = pl.ds(own_half, half), pl.ds(other_half, half)
        part[last - 1, rest, cols] = (
            wide(part[last - 1, rest, cols]) + wide(theirs[last - 1, rest, cols])
        ).astype(part.dtype)
        reduce_first(f).wait_recv()
        part[last - 1, at, cols] = (
            wide(part[last - 1, at, cols])
            + wide(theirs[last - 1, at, cols])
            + wide(sums[0, at, cols])
        ).astype(part.dtype)
        reduce(1, f).start()

    @pl.loop(2, steps)
    def _(j):
        k = last - j
        hand(k + 1).wait_recv()
        for f in range(CHUNKS):
            cols = column(f)
            base = wide(part[k, pl.ds(0, count), cols]) + wide(theirs[k, :, cols])
            reduce(j - 1, f).wait_recv()
            part[k, pl.ds(0, count), cols] = (base + wide(sums[j - 1, :, cols])).astype(part.dtype)

            @pl.when(j == 2)
            def _():
                reduce_first(f).wait_send()

            @pl.when(j > 2)
            def _():
                reduce(j - 2, f).wait_send()

            reduce(j, f).start()

    for f in range(CHUNKS):
        cols = column(f)
        base = wide(part[last, pl.ds(count, count), cols])
        reduce(last, f).wait_recv()
        total = base + wide(sums[last, :, cols])
        if f < CHUNKS // 2:
            swap_out[:, f * span : (f + 1) * span] = total.astype(swap_out.dtype)
            finish(f).start()
        else:
            i = f - CHUNKS // 2
            at = slice(i * span, (i + 1) * span)
            finish(i).wait_recv()
            out[:, at] = (total + wide(swap_in[:, at])).astype(out.dtype)

    for f in range(CHUNKS):
        gather(last, f).wait_send()
        gather_half(f).wait_send()
        reduce(last - 1, f).wait_send()
        reduce(last, f).wait_send()
    gather_coef(last).wait_send()
    gather_coef(steps).wait_send()
    swap(last).wait_send()
    swap_half().wait_send()
    swap_coef(last - 1).wait_send()
    swap_coef(last).wait_send()
    hand(last - 1).wait_send()
    hand(last).wait_send()
    for q in range(2):
        hand_half(q).wait_send()
    for i in range(CHUNKS // 2):
        finish(i).wait_send()


def local(
    n, tokens, routes, route_weight, gate_code, gate_scale, up_code, up_scale, down_code, down_scale
):
    steps = n // 2
    count, width = tokens.shape
    units = gate_code.shape[1]
    vmem = pl.BlockSpec(memory_space=pltpu.VMEM)
    far = pl.BlockSpec(memory_space=pl.ANY)
    bf16, f32 = jnp.bfloat16, jnp.float32
    dma = pltpu.SemaphoreType.DMA
    return pl.pallas_call(
        functools.partial(kernel, n),
        out_shape=jax.ShapeDtypeStruct((count, width // 2), bf16),
        in_specs=[far, vmem, vmem, far, far, far, far, far, far],
        out_specs=vmem,
        scratch_shapes=[
            pltpu.VMEM((steps, 2 * count, width), bf16),
            pltpu.VMEM((steps, 2 * count, width), bf16),
            pltpu.VMEM((steps, count, width), bf16),
            pltpu.VMEM((steps, count, width), bf16),
            pltpu.VMEM(gate_code.shape, bf16),
            pltpu.VMEM(up_code.shape, bf16),
            pltpu.VMEM(down_code.shape, bf16),
            pltpu.VMEM(gate_scale.shape[::-1], f32),
            pltpu.VMEM(up_scale.shape[::-1], f32),
            pltpu.VMEM(down_scale.shape[::-1], f32),
            pltpu.VMEM((2 * count, units), bf16),
            pltpu.VMEM((steps, 2, 8, 128), f32),
            pltpu.VMEM((count, width // 2), bf16),
            pltpu.VMEM((count, width // 2), bf16),
            dma((7,)),
            dma((2, CHUNKS)),
            dma((steps, CHUNKS)),
            dma((2,)),
            dma((steps,)),
            dma((2,)),
            dma((steps,)),
            dma((2,)),
            dma((steps,)),
            dma((4,)),
            dma((steps + 1,)),
            dma((2, CHUNKS)),
            dma((steps, CHUNKS)),
            dma((CHUNKS // 2,)),
            dma((CHUNKS // 2,)),
        ],
        compiler_params=pltpu.CompilerParams(
            collective_id=0, has_side_effects=True, vmem_limit_bytes=62 << 20
        ),
    )(
        tokens, routes.T, route_weight.T, gate_code, gate_scale.T, up_code, up_scale.T,
        down_code, down_scale.T,
    )


def solution(mesh):
    placed = (
        P(("rep", "ep"), None),
        P(("rep", "ep"), None),
        P(("rep", "ep"), None),
        P(None, ("ep", "tp")),
        P(None, ("ep", "tp")),
        P(None, ("ep", "tp")),
        P(None, ("ep", "tp")),
        P(("ep", "tp"), None),
        P(("ep", "tp"), None),
    )
    return jax.shard_map(
        functools.partial(local, mesh.shape["ep"]),
        mesh=mesh,
        in_specs=placed,
        out_specs=P(("rep", "ep"), "tp"),
        check_vma=False,
    )
```

```python
import functools

import jax
import jax.numpy as jnp
from jax import lax
from jax.experimental import pallas as pl
from jax.experimental.pallas import tpu as pltpu
from jax.sharding import PartitionSpec as P

EXPERTS = 4
QB = 128
CHUNKS = 8
PIECES = 4
MESH = pl.DeviceIdType.MESH


def kernel(
    n,
    tokens, routes, weights, gate_code, gate_scale, up_code, up_scale, down_code, down_scale,
    out,
    rows, part, theirs, sums, w_gate, w_up, w_down, s_gate, s_up, s_down,
    hidden, coef, swap_out, swap_in, route, weight,
    load_sem, ag_send, ag_recv, cf_send, cf_recv, sw_send, sw_recv, sc_send, sc_recv,
    sh_send, sh_recv, po_send, po_recv, rs_send, rs_recv, fx_send, fx_recv,
):
    steps = n // 2
    count = rows.shape[1] // 2
    half = count // 2
    width = rows.shape[2]
    span = width // CHUNKS
    units = w_gate.shape[1]
    last = steps - 1

    ep = lax.axis_index("ep")
    tp = lax.axis_index("tp")
    toward = 1 - 2 * tp
    ahead = {"ep": lax.rem(ep + toward + n, n)}
    behind = {"ep": lax.rem(ep - toward + n, n)}
    partner = {"tp": 1 - tp}
    expert = ep // (n // EXPERTS)
    own_half = pl.multiple_of(half * tp, half)
    other_half = pl.multiple_of(half * (1 - tp), half)

    def send(src, dst, send_sem, recv_sem, where):
        return pltpu.make_async_remote_copy(
            src_ref=src, dst_ref=dst, send_sem=send_sem, recv_sem=recv_sem,
            device_id=where, device_id_type=MESH,
        )

    own = rows.at[last, pl.ds(count, count)]

    def gather(k, f):
        cols = pl.ds(f * span, span)
        if isinstance(k, int) and k == 1:
            src = own.at[:, cols]
        else:
            src = rows.at[k - 2, pl.ds(0, count), cols]
        return send(
            src, rows.at[k - 1, pl.ds(0, count), cols],
            ag_send.at[lax.rem(k, 2), f], ag_recv.at[k - 1, f], ahead,
        )

    def gather_half(f):
        cols = pl.ds(f * span, span)
        return send(
            rows.at[last - 1, pl.ds(own_half, half), cols], rows.at[last, pl.ds(0, half), cols],
            ag_send.at[steps % 2, f], ag_recv.at[last, f], ahead,
        )

    def gather_coef(k):
        src = coef.at[last, 1] if isinstance(k, int) and k == 1 else coef.at[k - 2, 0]
        return send(
            src, coef.at[k - 1, 0], cf_send.at[lax.rem(k, 2)], cf_recv.at[k - 1], ahead
        )

    def swap(k):
        return send(
            rows.at[k - 1, pl.ds(0, count)], rows.at[k - 1, pl.ds(count, count)],
            sw_send.at[lax.rem(k, 2)], sw_recv.at[k - 1], partner,
        )

    def swap_half(f):
        cols = pl.ds(f * span, span)
        return send(
            rows.at[last, pl.ds(0, half), cols], rows.at[last, pl.ds(half, half), cols],
            sh_send.at[f], sh_recv.at[f], partner,
        )

    def swap_coef(k):
        return send(
            coef.at[k - 1, 0], coef.at[k - 1, 1],
            sc_send.at[lax.rem(k, 2)], sc_recv.at[k - 1], partner,
        )

    def hand(k):
        return send(
            part.at[k - 1, pl.ds(count, count)], theirs.at[k - 1],
            po_send.at[lax.rem(k, 2)], po_recv.at[k - 1], partner,
        )

    def hand_half(q):
        cols = pl.ds(pl.multiple_of(q * (width // 2), width // 2), width // 2)
        return send(
            part.at[last, pl.ds(half, half), cols], theirs.at[last, pl.ds(0, half), cols],
            po_send.at[2 + q], po_recv.at[last + q], partner,
        )

    def column(f):
        chunk = lax.rem(CHUNKS // 2 * (1 - tp) + f, CHUNKS)
        return pl.ds(pl.multiple_of(chunk * span, span), span)

    def reduce(j, f):
        return send(
            part.at[last - j, pl.ds(0, count), column(f)], sums.at[j, :, column(f)],
            rs_send.at[lax.rem(j, 2), f], rs_recv.at[j, f], behind,
        )

    def reduce_first(f):
        return send(
            part.at[last, pl.ds(0, half), column(f)],
            sums.at[0, pl.ds(own_half, half), column(f)],
            rs_send.at[0, f], rs_recv.at[0, f], behind,
        )

    def finish(i):
        cols = pl.ds(i * span, span)
        return send(
            swap_out.at[:, cols], swap_in.at[:, cols], fx_send.at[i], fx_recv.at[i], partner
        )

    def when(test, do):
        if isinstance(test, bool):
            if test:
                do()
        else:
            pl.when(test)(do)

    loads = [
        pltpu.make_async_copy(src, dst, load_sem.at[i])
        for i, (src, dst) in enumerate((
            (tokens, own), (gate_scale, s_gate), (gate_code, w_gate), (up_scale, s_up),
            (up_code, w_up), (down_scale, s_down), (down_code, w_down),
            (routes, route), (weights, weight),
        ))
    ]
    for i in (0, 7, 8):
        loads[i].start()

    barrier = pltpu.get_barrier_semaphore()
    for device in (ahead, behind, partner):
        pl.semaphore_signal(barrier, inc=1, device_id=device, device_id_type=MESH)
    pl.semaphore_wait(barrier, 3)
    loads[0].wait()
    for f in range(CHUNKS):
        gather(1, f).start()

    for load in loads[1:7]:
        load.start()
    loads[7].wait()
    loads[8].wait()
    names = lax.broadcasted_iota(jnp.int32, (8, count), 0)
    mine = jnp.where(names == route[0:1, :], weight[0:1, :], 0.0)
    mine += jnp.where(names == route[1:2, :], weight[1:2, :], 0.0)
    coef[last, 1] = jnp.concatenate((mine, jnp.zeros((8, 128 - count), jnp.float32)), axis=1)
    gather_coef(1).start()

    def poll(k, f):
        def full():
            gather(k, f).wait_recv()
            if isinstance(k, int):
                if k >= 2:
                    gather(k - 1, f).wait_send()
                gather(k + 1, f).start()
                return

            @pl.when(k < last)
            def _():
                gather(k - 1, f).wait_send()
                gather(k + 1, f).start()

            @pl.when(k == last)
            def _():
                gather(k - 1, f).wait_send()
                gather_half(f).start()

        def half_too():
            gather_half(f).wait_recv()
            swap_half(f).start()

        def weights_too():
            gather_coef(k).wait_recv()

            def onward():
                if not isinstance(k, int) or k >= 2:
                    gather_coef(k - 1).wait_send()
                gather_coef(k + 1).start()

            when(k < steps, onward)

        def across():
            if not isinstance(k, int) or k >= 3:
                swap(k - 2).wait_send()
                swap_coef(k - 2).wait_send()
            swap(k).start()
            swap_coef(k).start()

        when(k < steps, full)
        when(k == steps, half_too)
        if f == CHUNKS - 1:
            weights_too()
            when(k < steps, across)

    def polls(k, p):
        for f in range(CHUNKS // PIECES):
            poll(k, p * (CHUNKS // PIECES) + f)

    def dequant(code, scale, base):
        blocks = code.shape[1] // QB
        grid = scale[:, pl.ds(base, QB)]
        if blocks % 8:
            pad = jnp.zeros((8 - blocks % 8, QB), jnp.float32)
            grid = jnp.concatenate((grid, pad), axis=0)
        grid = grid.T
        for b in range(blocks):
            at = (pl.ds(base, QB), pl.ds(b * QB, QB))
            code[at] = (code[at].astype(jnp.float32) * grid[:, b : b + 1]).astype(code.dtype)

    def dequant_piece(m, f):
        code, scale = ((w_gate, s_gate), (w_up, s_up), (w_down, s_down))[m]
        size = code.shape[0] // PIECES

        @pl.loop(0, size // QB)
        def _(r):
            dequant(code, scale, pl.multiple_of(f * size + r * QB, QB))

    def arrived(k):
        swap(k).wait_recv()
        swap_coef(k).wait_recv()

    def factors(line, shift):
        token = lax.broadcasted_iota(jnp.int32, (count, 128), 0)
        lane = lax.broadcasted_iota(jnp.int32, (count, 128), 1)
        return jnp.sum(
            jnp.where(lane == ((token + shift) & (count - 1)), line, 0.0), axis=1, keepdims=True
        )

    def line(k, side):
        return coef[k - 1, side, pl.ds(expert, 1), :]

    def widen(k, p, low, size, factor):
        cols = pl.ds(p * (units // 2), units // 2)
        x = rows[k - 1, low : low + size]
        gate = jnp.dot(x, w_gate[:, cols], preferred_element_type=jnp.float32)
        up = jnp.dot(x, w_up[:, cols], preferred_element_type=jnp.float32)
        small = jnp.exp(-jnp.abs(gate))
        silu = gate * (jnp.where(gate >= 0, 1.0, small) / (1.0 + small))
        hidden[low : low + size, cols] = (silu * up * factor()).astype(hidden.dtype)

    def narrow(k, q, low, size):
        cols = pl.ds(pl.multiple_of(q * (width // 2), width // 2), width // 2)
        got = jnp.dot(
            hidden[low : low + size], w_down[:, cols], preferred_element_type=jnp.float32
        )
        part[k - 1, low : low + size, cols] = got.astype(part.dtype)

    def pieces(k):
        def both():
            return jnp.concatenate((factors(line(k, 0), 0), factors(line(k, 1), 0)), axis=0)

        def give():
            narrow(k, 1, 0, 2 * count)

            @pl.when(k >= 3)
            def _():
                hand(k - 2).wait_send()

            hand(k).start()

        return [
            lambda: arrived(k),
            lambda: widen(k, 0, 0, 2 * count, both),
            lambda: widen(k, 1, 0, 2 * count, both),
            lambda: narrow(k, 0, 0, 2 * count),
            give,
        ]

    for k in range(1, 4):
        loads[2 * k - 1].wait()
        loads[2 * k].wait()
        for p in range(PIECES):
            polls(k, p)
            dequant_piece(k - 1, p)

    @pl.loop(4, 6)
    def _(k):
        todo = pieces(2 * k - 7) + pieces(2 * k - 6)
        polls(k, 0)
        for do in todo[0:3]:
            do()
        polls(k, 1)
        for do in todo[3:5]:
            do()
        polls(k, 2)
        for do in todo[5:8]:
            do()
        polls(k, 3)
        for do in todo[8:10]:
            do()

    @pl.loop(6, steps + 1)
    def _(k):
        ready, *todo = pieces(k - 1)
        for p in range(PIECES):
            polls(k, p)
            if p == 0:
                ready()
            todo[p]()

    def wide(ref):
        return ref.astype(jnp.float32)

    for f in range(CHUNKS):
        swap_half(f).wait_recv()
    for p in range(2):
        widen(steps, p, 0, count, lambda: factors(line(steps, 0), half * tp))
    for q in (tp, 1 - tp):
        narrow(steps, q, 0, count)
        hand_half(q).start()
    for f in range(CHUNKS):
        if f == 0:
            hand_half(1 - tp).wait_recv()
        if f == CHUNKS // 2:
            hand_half(tp).wait_recv()
        cols = column(f)
        part[last, pl.ds(0, half), cols] = (
            wide(part[last, pl.ds(0, half), cols]) + wide(theirs[last, pl.ds(0, half), cols])
        ).astype(part.dtype)
        reduce_first(f).start()
    for p in range(2):
        widen(steps, p, count, count, lambda: factors(line(steps, 1), 0))
    for q in range(2):
        narrow(steps, q, count, count)

    hand(last).wait_recv()
    for f in range(CHUNKS):
        cols = column(f)
        at, rest = pl.ds(own_half, half), pl.ds(other_half, half)
        part[last - 1, rest, cols] = (
            wide(part[last - 1, rest, cols]) + wide(theirs[last - 1, rest, cols])
        ).astype(part.dtype)
        reduce_first(f).wait_recv()
        part[last - 1, at, cols] = (
            wide(part[last - 1, at, cols])
            + wide(theirs[last - 1, at, cols])
            + wide(sums[0, at, cols])
        ).astype(part.dtype)
        reduce(1, f).start()

    @pl.loop(2, steps)
    def _(j):
        k = last - j
        hand(k + 1).wait_recv()
        for f in range(CHUNKS):
            cols = column(f)
            base = wide(part[k, pl.ds(0, count), cols]) + wide(theirs[k, :, cols])
            reduce(j - 1, f).wait_recv()
            part[k, pl.ds(0, count), cols] = (base + wide(sums[j - 1, :, cols])).astype(part.dtype)

            @pl.when(j == 2)
            def _():
                reduce_first(f).wait_send()

            @pl.when(j > 2)
            def _():
                reduce(j - 2, f).wait_send()

            reduce(j, f).start()

    for f in range(CHUNKS):
        cols = column(f)
        base = wide(part[last, pl.ds(count, count), cols])
        reduce(last, f).wait_recv()
        total = base + wide(sums[last, :, cols])
        if f < CHUNKS // 2:
            swap_out[:, f * span : (f + 1) * span] = total.astype(swap_out.dtype)
            finish(f).start()
        else:
            i = f - CHUNKS // 2
            at = slice(i * span, (i + 1) * span)
            finish(i).wait_recv()
            out[:, at] = (total + wide(swap_in[:, at])).astype(out.dtype)

    for f in range(CHUNKS):
        gather(last, f).wait_send()
        gather_half(f).wait_send()
        reduce(last - 1, f).wait_send()
        reduce(last, f).wait_send()
        swap_half(f).wait_send()
    gather_coef(last).wait_send()
    gather_coef(steps).wait_send()
    swap(last).wait_send()
    swap(last - 1).wait_send()
    swap_coef(last - 1).wait_send()
    swap_coef(last).wait_send()
    hand(last - 1).wait_send()
    hand(last).wait_send()
    for q in range(2):
        hand_half(q).wait_send()
    for i in range(CHUNKS // 2):
        finish(i).wait_send()


def local(
    n, tokens, routes, route_weight, gate_code, gate_scale, up_code, up_scale, down_code, down_scale
):
    steps = n // 2
    count, width = tokens.shape
    units = gate_code.shape[1]
    vmem = pl.BlockSpec(memory_space=pltpu.VMEM)
    far = pl.BlockSpec(memory_space=pl.ANY)
    bf16, f32 = jnp.bfloat16, jnp.float32
    dma = pltpu.SemaphoreType.DMA
    return pl.pallas_call(
        functools.partial(kernel, n),
        out_shape=jax.ShapeDtypeStruct((count, width // 2), bf16),
        in_specs=[far] * 9,
        out_specs=vmem,
        scratch_shapes=[
            pltpu.VMEM((steps, 2 * count, width), bf16),
            pltpu.VMEM((steps, 2 * count, width), bf16),
            pltpu.VMEM((steps, count, width), bf16),
            pltpu.VMEM((steps, count, width), bf16),
            pltpu.VMEM(gate_code.shape, bf16),
            pltpu.VMEM(up_code.shape, bf16),
            pltpu.VMEM(down_code.shape, bf16),
            pltpu.VMEM(gate_scale.shape[::-1], f32),
            pltpu.VMEM(up_scale.shape[::-1], f32),
            pltpu.VMEM(down_scale.shape[::-1], f32),
            pltpu.VMEM((2 * count, units), bf16),
            pltpu.VMEM((steps, 2, 8, 128), f32),
            pltpu.VMEM((count, width // 2), bf16),
            pltpu.VMEM((count, width // 2), bf16),
            pltpu.VMEM((2, count), jnp.int32),
            pltpu.VMEM((2, count), f32),
            dma((9,)),
            dma((2, CHUNKS)),
            dma((steps, CHUNKS)),
            dma((2,)),
            dma((steps,)),
            dma((2,)),
            dma((steps,)),
            dma((2,)),
            dma((steps,)),
            dma((CHUNKS,)),
            dma((CHUNKS,)),
            dma((4,)),
            dma((steps + 1,)),
            dma((2, CHUNKS)),
            dma((steps, CHUNKS)),
            dma((CHUNKS // 2,)),
            dma((CHUNKS // 2,)),
        ],
        compiler_params=pltpu.CompilerParams(
            collective_id=0, has_side_effects=True, vmem_limit_bytes=62 << 20
        ),
    )(
        tokens, routes.T, route_weight.T, gate_code, gate_scale.T, up_code, up_scale.T,
        down_code, down_scale.T,
    )


def solution(mesh):
    placed = (
        P(("rep", "ep"), None),
        P(("rep", "ep"), None),
        P(("rep", "ep"), None),
        P(None, ("ep", "tp")),
        P(None, ("ep", "tp")),
        P(None, ("ep", "tp")),
        P(None, ("ep", "tp")),
        P(("ep", "tp"), None),
        P(("ep", "tp"), None),
    )
    return jax.shard_map(
        functools.partial(local, mesh.shape["ep"]),
        mesh=mesh,
        in_specs=placed,
        out_specs=P(("rep", "ep"), "tp"),
        check_vma=False,
    )
```

```python
import functools

import jax
import jax.numpy as jnp
from jax import lax
from jax.experimental import pallas as pl
from jax.experimental.pallas import tpu as pltpu
from jax.sharding import PartitionSpec as P

EXPERTS = 4
QB = 128
CHUNKS = 8
PIECES = 4
MESH = pl.DeviceIdType.MESH


def kernel(
    n,
    tokens, routes, weights, gate_code, gate_scale, up_code, up_scale, down_code, down_scale,
    out,
    rows, part, theirs, sums, w_gate, w_up, w_down, s_gate, s_up, s_down,
    hidden, coef, swap_out, swap_in, route, weight, gate_sum, up_sum,
    load_sem, ag_send, ag_recv, cf_send, cf_recv, sw_send, sw_recv, sc_send, sc_recv,
    sh_send, sh_recv, po_send, po_recv, rs_send, rs_recv, fx_send, fx_recv,
):
    steps = n // 2
    count = rows.shape[1] // 2
    half = count // 2
    width = rows.shape[2]
    span = width // CHUNKS
    units = w_gate.shape[1]
    last = steps - 1

    ep = lax.axis_index("ep")
    tp = lax.axis_index("tp")
    toward = 1 - 2 * tp
    ahead = {"ep": lax.rem(ep + toward + n, n)}
    behind = {"ep": lax.rem(ep - toward + n, n)}
    partner = {"tp": 1 - tp}
    expert = ep // (n // EXPERTS)
    own_half = pl.multiple_of(half * tp, half)
    other_half = pl.multiple_of(half * (1 - tp), half)

    def send(src, dst, send_sem, recv_sem, where):
        return pltpu.make_async_remote_copy(
            src_ref=src, dst_ref=dst, send_sem=send_sem, recv_sem=recv_sem,
            device_id=where, device_id_type=MESH,
        )

    own = rows.at[last, pl.ds(count, count)]

    def gather(k, f):
        cols = pl.ds(f * span, span)
        if isinstance(k, int) and k == 1:
            src = own.at[:, cols]
        else:
            src = rows.at[k - 2, pl.ds(0, count), cols]
        return send(
            src, rows.at[k - 1, pl.ds(0, count), cols],
            ag_send.at[lax.rem(k, 2), f], ag_recv.at[k - 1, f], ahead,
        )

    def gather_half(f):
        cols = pl.ds(f * span, span)
        return send(
            rows.at[last - 1, pl.ds(own_half, half), cols], rows.at[last, pl.ds(0, half), cols],
            ag_send.at[steps % 2, f], ag_recv.at[last, f], ahead,
        )

    def gather_coef(k):
        src = coef.at[last, 1] if isinstance(k, int) and k == 1 else coef.at[k - 2, 0]
        return send(
            src, coef.at[k - 1, 0], cf_send.at[lax.rem(k, 2)], cf_recv.at[k - 1], ahead
        )

    def swap(k):
        return send(
            rows.at[k - 1, pl.ds(0, count)], rows.at[k - 1, pl.ds(count, count)],
            sw_send.at[lax.rem(k, 2)], sw_recv.at[k - 1], partner,
        )

    def swap_half(f):
        cols = pl.ds(f * span, span)
        return send(
            rows.at[last, pl.ds(0, half), cols], rows.at[last, pl.ds(half, half), cols],
            sh_send.at[f], sh_recv.at[f], partner,
        )

    def swap_coef(k):
        return send(
            coef.at[k - 1, 0], coef.at[k - 1, 1],
            sc_send.at[lax.rem(k, 2)], sc_recv.at[k - 1], partner,
        )

    def hand(k):
        return send(
            part.at[k - 1, pl.ds(count, count)], theirs.at[k - 1],
            po_send.at[lax.rem(k, 2)], po_recv.at[k - 1], partner,
        )

    def hand_half(q):
        cols = pl.ds(pl.multiple_of(q * (width // 2), width // 2), width // 2)
        return send(
            part.at[last, pl.ds(half, half), cols], theirs.at[last, pl.ds(0, half), cols],
            po_send.at[2 + q], po_recv.at[last + q], partner,
        )

    def column(f):
        chunk = lax.rem(CHUNKS // 2 * (1 - tp) + f, CHUNKS)
        return pl.ds(pl.multiple_of(chunk * span, span), span)

    def reduce(j, f):
        return send(
            part.at[last - j, pl.ds(0, count), column(f)], sums.at[j, :, column(f)],
            rs_send.at[lax.rem(j, 2), f], rs_recv.at[j, f], behind,
        )

    def reduce_first(f):
        return send(
            part.at[last, pl.ds(0, half), column(f)],
            sums.at[0, pl.ds(own_half, half), column(f)],
            rs_send.at[0, f], rs_recv.at[0, f], behind,
        )

    def finish(i):
        cols = pl.ds(i * span, span)
        return send(
            swap_out.at[:, cols], swap_in.at[:, cols], fx_send.at[i], fx_recv.at[i], partner
        )

    def when(test, do):
        if isinstance(test, bool):
            if test:
                do()
        else:
            pl.when(test)(do)

    loads = [
        pltpu.make_async_copy(src, dst, load_sem.at[i])
        for i, (src, dst) in enumerate((
            (tokens, own), (gate_scale, s_gate), (gate_code, w_gate), (up_scale, s_up),
            (up_code, w_up), (down_scale, s_down), (down_code, w_down),
            (routes, route), (weights, weight),
        ))
    ]
    for i in (0, 7, 8):
        loads[i].start()

    barrier = pltpu.get_barrier_semaphore()
    for device in (ahead, behind, partner):
        pl.semaphore_signal(barrier, inc=1, device_id=device, device_id_type=MESH)
    pl.semaphore_wait(barrier, 3)
    loads[0].wait()
    for f in range(CHUNKS):
        gather(1, f).start()

    for load in loads[1:7]:
        load.start()
    loads[7].wait()
    loads[8].wait()
    twice = [jnp.concatenate((route[i : i + 1, :],) * 2, axis=1) for i in range(2)]
    shares = [jnp.concatenate((weight[i : i + 1, :],) * 2, axis=1) for i in range(2)]
    names = 2 * lax.broadcasted_iota(jnp.int32, (2, 2 * count), 0)
    names += jnp.where(lax.broadcasted_iota(jnp.int32, (2, 2 * count), 1) >= count, 1, 0)
    coef[last, 1] = jnp.where(names == twice[0], shares[0], 0.0) + jnp.where(
        names == twice[1], shares[1], 0.0
    )
    gather_coef(1).start()

    def poll(k, f):
        def full():
            gather(k, f).wait_recv()
            if isinstance(k, int):
                if k >= 2:
                    gather(k - 1, f).wait_send()
                gather(k + 1, f).start()
                return

            @pl.when(k < last)
            def _():
                gather(k - 1, f).wait_send()
                gather(k + 1, f).start()

            @pl.when(k == last)
            def _():
                gather(k - 1, f).wait_send()
                gather_half(f).start()

        def half_too():
            gather_half(f).wait_recv()
            swap_half(f).start()

        def weights_too():
            gather_coef(k).wait_recv()

            def onward():
                if not isinstance(k, int) or k >= 2:
                    gather_coef(k - 1).wait_send()
                gather_coef(k + 1).start()

            when(k < steps, onward)

        def across():
            if not isinstance(k, int) or k >= 3:
                swap(k - 2).wait_send()
                swap_coef(k - 2).wait_send()
            swap(k).start()
            swap_coef(k).start()

        when(k < steps, full)
        when(k == steps, half_too)
        if f == CHUNKS - 1:
            weights_too()
            when(k < steps, across)

    def polls(k, p):
        for f in range(CHUNKS // PIECES):
            poll(k, p * (CHUNKS // PIECES) + f)

    def dequant(code, scale, base):
        blocks = code.shape[1] // QB
        grid = scale[:, pl.ds(base, QB)]
        if blocks % 8:
            pad = jnp.zeros((8 - blocks % 8, QB), jnp.float32)
            grid = jnp.concatenate((grid, pad), axis=0)
        grid = grid.T
        for b in range(blocks):
            at = (pl.ds(base, QB), pl.ds(b * QB, QB))
            code[at] = (code[at].astype(jnp.float32) * grid[:, b : b + 1]).astype(code.dtype)

    def dequant_piece(m, f):
        code, scale = ((w_gate, s_gate), (w_up, s_up), (w_down, s_down))[m]
        size = code.shape[0] // PIECES

        @pl.loop(0, size // QB)
        def _(r):
            dequant(code, scale, pl.multiple_of(f * size + r * QB, QB))

    def arrived(k):
        swap(k).wait_recv()
        swap_coef(k).wait_recv()

    def factors(line, shift):
        token = lax.broadcasted_iota(jnp.int32, (count, 128), 0)
        lane = lax.broadcasted_iota(jnp.int32, (count, 128), 1)
        return jnp.sum(
            jnp.where(lane == ((token + shift) & (count - 1)) + count * lax.rem(expert, 2), line, 0.0),
            axis=1,
            keepdims=True,
        )

    def line(k, side):
        return coef[k - 1, side, pl.ds(expert // 2, 1), :]

    def gated(gate, up):
        small = jnp.exp(-jnp.abs(gate))
        return gate * (jnp.where(gate >= 0, 1.0, small) / (1.0 + small)) * up

    def widen(k, p, low, size, factor):
        cols = pl.ds(p * (units // 2), units // 2)
        x = rows[k - 1, low : low + size]
        gate = jnp.dot(x, w_gate[:, cols], preferred_element_type=jnp.float32)
        up = jnp.dot(x, w_up[:, cols], preferred_element_type=jnp.float32)
        hidden[low : low + size, cols] = (gated(gate, up) * factor()).astype(hidden.dtype)

    def narrow(k, q, low, size):
        cols = pl.ds(pl.multiple_of(q * (width // 2), width // 2), width // 2)
        got = jnp.dot(
            hidden[low : low + size], w_down[:, cols], preferred_element_type=jnp.float32
        )
        part[k - 1, low : low + size, cols] = got.astype(part.dtype)

    def pieces(k):
        def both():
            return jnp.concatenate((factors(line(k, 0), 0), factors(line(k, 1), 0)), axis=0)

        def give():
            narrow(k, 1, 0, 2 * count)

            @pl.when(k >= 3)
            def _():
                hand(k - 2).wait_send()

            hand(k).start()

        return [
            lambda: arrived(k),
            lambda: widen(k, 0, 0, 2 * count, both),
            lambda: widen(k, 1, 0, 2 * count, both),
            lambda: narrow(k, 0, 0, 2 * count),
            give,
        ]

    for k in range(1, 4):
        loads[2 * k - 1].wait()
        loads[2 * k].wait()
        for p in range(PIECES):
            polls(k, p)
            dequant_piece(k - 1, p)

    @pl.loop(4, 6)
    def _(k):
        todo = pieces(2 * k - 7) + pieces(2 * k - 6)
        polls(k, 0)
        for do in todo[0:3]:
            do()
        polls(k, 1)
        for do in todo[3:5]:
            do()
        polls(k, 2)
        for do in todo[5:8]:
            do()
        polls(k, 3)
        for do in todo[8:10]:
            do()

    @pl.loop(6, steps + 1)
    def _(k):
        ready, *todo = pieces(k - 1)
        for p in range(PIECES):
            polls(k, p)
            if p == 0:
                ready()
            todo[p]()

    def wide(ref):
        return ref.astype(jnp.float32)

    for g in range(PIECES):
        for f in range(CHUNKS // PIECES):
            swap_half(g * (CHUNKS // PIECES) + f).wait_recv()
        depth = slice(g * (width // PIECES), (g + 1) * (width // PIECES))
        x = rows[last, 0:count, depth]
        for acc, w in ((gate_sum, w_gate), (up_sum, w_up)):
            got = jnp.dot(x, w[depth, :], preferred_element_type=jnp.float32)
            acc[...] = got if g == 0 else acc[...] + got
    hidden[0:count, :] = (
        gated(gate_sum[...], up_sum[...]) * factors(line(steps, 0), half * tp)
    ).astype(hidden.dtype)
    for q in (tp, 1 - tp):
        narrow(steps, q, 0, count)
        hand_half(q).start()
    for f in range(CHUNKS):
        if f == 0:
            hand_half(1 - tp).wait_recv()
        if f == CHUNKS // 2:
            hand_half(tp).wait_recv()
        cols = column(f)
        part[last, pl.ds(0, half), cols] = (
            wide(part[last, pl.ds(0, half), cols]) + wide(theirs[last, pl.ds(0, half), cols])
        ).astype(part.dtype)
        reduce_first(f).start()
    for p in range(2):
        widen(steps, p, count, count, lambda: factors(line(steps, 1), 0))
    for q in range(2):
        narrow(steps, q, count, count)

    hand(last).wait_recv()
    for f in range(CHUNKS):
        cols = column(f)
        at, rest = pl.ds(own_half, half), pl.ds(other_half, half)
        part[last - 1, rest, cols] = (
            wide(part[last - 1, rest, cols]) + wide(theirs[last - 1, rest, cols])
        ).astype(part.dtype)
        reduce_first(f).wait_recv()
        part[last - 1, at, cols] = (
            wide(part[last - 1, at, cols])
            + wide(theirs[last - 1, at, cols])
            + wide(sums[0, at, cols])
        ).astype(part.dtype)
        reduce(1, f).start()

    @pl.loop(2, steps)
    def _(j):
        k = last - j
        hand(k + 1).wait_recv()
        for f in range(CHUNKS):
            cols = column(f)
            base = wide(part[k, pl.ds(0, count), cols]) + wide(theirs[k, :, cols])
            reduce(j - 1, f).wait_recv()
            part[k, pl.ds(0, count), cols] = (base + wide(sums[j - 1, :, cols])).astype(part.dtype)

            @pl.when(j == 2)
            def _():
                reduce_first(f).wait_send()

            @pl.when(j > 2)
            def _():
                reduce(j - 2, f).wait_send()

            reduce(j, f).start()

    for f in range(CHUNKS):
        cols = column(f)
        base = wide(part[last, pl.ds(count, count), cols])
        reduce(last, f).wait_recv()
        total = base + wide(sums[last, :, cols])
        if f < CHUNKS // 2:
            swap_out[:, f * span : (f + 1) * span] = total.astype(swap_out.dtype)
            finish(f).start()
        else:
            i = f - CHUNKS // 2
            at = slice(i * span, (i + 1) * span)
            finish(i).wait_recv()
            out[:, at] = (total + wide(swap_in[:, at])).astype(out.dtype)

    for f in range(CHUNKS):
        gather(last, f).wait_send()
        gather_half(f).wait_send()
        reduce(last - 1, f).wait_send()
        reduce(last, f).wait_send()
        swap_half(f).wait_send()
    gather_coef(last).wait_send()
    gather_coef(steps).wait_send()
    swap(last).wait_send()
    swap(last - 1).wait_send()
    swap_coef(last - 1).wait_send()
    swap_coef(last).wait_send()
    hand(last - 1).wait_send()
    hand(last).wait_send()
    for q in range(2):
        hand_half(q).wait_send()
    for i in range(CHUNKS // 2):
        finish(i).wait_send()


def local(
    n, tokens, routes, route_weight, gate_code, gate_scale, up_code, up_scale, down_code, down_scale
):
    steps = n // 2
    count, width = tokens.shape
    units = gate_code.shape[1]
    vmem = pl.BlockSpec(memory_space=pltpu.VMEM)
    far = pl.BlockSpec(memory_space=pl.ANY)
    bf16, f32 = jnp.bfloat16, jnp.float32
    dma = pltpu.SemaphoreType.DMA
    return pl.pallas_call(
        functools.partial(kernel, n),
        out_shape=jax.ShapeDtypeStruct((count, width // 2), bf16),
        in_specs=[far] * 9,
        out_specs=vmem,
        scratch_shapes=[
            pltpu.VMEM((steps, 2 * count, width), bf16),
            pltpu.VMEM((steps, 2 * count, width), bf16),
            pltpu.VMEM((steps, count, width), bf16),
            pltpu.VMEM((steps, count, width), bf16),
            pltpu.VMEM(gate_code.shape, bf16),
            pltpu.VMEM(up_code.shape, bf16),
            pltpu.VMEM(down_code.shape, bf16),
            pltpu.VMEM(gate_scale.shape[::-1], f32),
            pltpu.VMEM(up_scale.shape[::-1], f32),
            pltpu.VMEM(down_scale.shape[::-1], f32),
            pltpu.VMEM((2 * count, units), bf16),
            pltpu.VMEM((steps, 2, 2, 2 * count), f32),
            pltpu.VMEM((count, width // 2), bf16),
            pltpu.VMEM((count, width // 2), bf16),
            pltpu.VMEM((2, count), jnp.int32),
            pltpu.VMEM((2, count), f32),
            pltpu.VMEM((count, units), f32),
            pltpu.VMEM((count, units), f32),
            dma((9,)),
            dma((2, CHUNKS)),
            dma((steps, CHUNKS)),
            dma((2,)),
            dma((steps,)),
            dma((2,)),
            dma((steps,)),
            dma((2,)),
            dma((steps,)),
            dma((CHUNKS,)),
            dma((CHUNKS,)),
            dma((4,)),
            dma((steps + 1,)),
            dma((2, CHUNKS)),
            dma((steps, CHUNKS)),
            dma((CHUNKS // 2,)),
            dma((CHUNKS // 2,)),
        ],
        compiler_params=pltpu.CompilerParams(
            collective_id=0, has_side_effects=True, vmem_limit_bytes=62 << 20
        ),
    )(
        tokens, routes.T, route_weight.T, gate_code, gate_scale.T, up_code, up_scale.T,
        down_code, down_scale.T,
    )


def solution(mesh):
    placed = (
        P(("rep", "ep"), None),
        P(("rep", "ep"), None),
        P(("rep", "ep"), None),
        P(None, ("ep", "tp")),
        P(None, ("ep", "tp")),
        P(None, ("ep", "tp")),
        P(None, ("ep", "tp")),
        P(("ep", "tp"), None),
        P(("ep", "tp"), None),
    )
    return jax.shard_map(
        functools.partial(local, mesh.shape["ep"]),
        mesh=mesh,
        in_specs=placed,
        out_specs=P(("rep", "ep"), "tp"),
        check_vma=False,
    )
```
